16 devices in a mesh: dp: 1, tp: 16 (over x, y, z, core).
Axes of the slice: x: 2, y: 2, z: 2, core: 2. Of those that a mesh axis runs over, the one named last changes fastest.
Arguments:
- x: bfloat16 [2048, 12288], P(('dp', 'tp'))
- gain: bfloat16 [12288], replicated
- wq: bfloat16 [12288, 12288], P(None, 'tp')
- wk: bfloat16 [12288, 12288], P(None, 'tp')
- wv: bfloat16 [12288, 12288], P(None, 'tp')
- wo: bfloat16 [12288, 12288], P('tp')
Outputs:
- output: bfloat16 [2048, 12288], P(('dp', 'tp'))
All inputs are finite; a program needn't handle non-finite values.
Results may differ from the reference program's by a relative error of at most 0.012.
Values are sent between devices in bfloat16 or wider.
A program may use at most 2 GiB of HBM per device.

```python
import jax
import jax.numpy as jnp
from jax import lax

ROWS = 2048
D = 12288
HEADS = 96
KV_HEADS = 96
HEAD = 128
THETA = 10000


def setup_inputs(seed: int = 0, part: int = 0) -> dict:
    kx, kn, kq, kk, kv, ko = jax.random.split(jax.random.key(seed), 6)

    def weights(key, rows, columns):
        return jax.random.normal(key, (rows, columns), jnp.float32) * rows**-0.5

    drawn = {
        "x": jax.random.normal(jax.random.fold_in(kx, part), (ROWS, D), jnp.float32),
        "gain": 1 + 0.1 * jax.random.normal(kn, (D,), jnp.float32),
        "wq": 2 * weights(kq, D, HEADS * HEAD),
        "wk": 2 * weights(kk, D, KV_HEADS * HEAD),
        "wv": 4 * weights(kv, D, KV_HEADS * HEAD),
        "wo": weights(ko, HEADS * HEAD, D),
    }
    return {k: v.astype(jnp.bfloat16) for k, v in drawn.items()}


def normed(x, gain):
    wide = x.astype(jnp.float32)
    scale = lax.rsqrt(jnp.mean(wide * wide, -1, keepdims=True) + 1e-6)
    return (wide * scale * gain.astype(jnp.float32)).astype(jnp.bfloat16)


def turned(t, place, theta):
    half = t.shape[-1] // 2
    angle = place.astype(jnp.float32)[:, None] * theta ** (-jnp.arange(half, dtype=jnp.float32) / half)
    cos, sin = jnp.cos(angle)[:, None], jnp.sin(angle)[:, None]
    a, b = t[..., :half].astype(jnp.float32), t[..., half:].astype(jnp.float32)
    return jnp.concatenate([a * cos - b * sin, b * cos + a * sin], -1).astype(jnp.bfloat16)


def matmul(a, w):
    return jnp.dot(a, w, preferred_element_type=jnp.float32).astype(jnp.bfloat16)


def einsum(form, a, b):
    return jnp.einsum(form, a.astype(jnp.float32), b.astype(jnp.float32))


def attention(q, k, v):
    scores = einsum("tgsd,ugd->gstu", q, k) * q.shape[-1] ** -0.5
    token = jnp.arange(q.shape[0])
    scores = jnp.where(token[:, None] >= token, scores, -jnp.inf)
    weights = jax.nn.softmax(scores, -1).astype(jnp.bfloat16)
    return einsum("gstu,ugd->tgsd", weights, v).astype(jnp.bfloat16)


def reference(x, gain, wq, wk, wv, wo):
    a, place = normed(x, gain), jnp.arange(ROWS)
    q = turned(matmul(a, wq).reshape(ROWS, HEADS, HEAD), place, THETA).reshape(ROWS, KV_HEADS, -1, HEAD)
    k = turned(matmul(a, wk).reshape(ROWS, KV_HEADS, HEAD), place, THETA)
    v = matmul(a, wv).reshape(ROWS, KV_HEADS, HEAD)
    seen = attention(q, k, v).reshape(ROWS, HEADS * HEAD)
    return (x.astype(jnp.float32) + jnp.dot(seen, wo, preferred_element_type=jnp.float32)).astype(jnp.bfloat16)
```

```python
import functools

import jax
import jax.numpy as jnp
from jax import lax
from jax.experimental import pallas as pl
from jax.experimental.pallas import tpu as pltpu
from jax.sharding import PartitionSpec as P


NEG = -1e30
HIDDEN = 2 * NEG
LOG2E = 1.4426950408889634
VMEM = 63 * 2**20
TILE = 2048
HEAD = 128
THETA = 10000
LINKS = (8, 4, 2)
FAR = 14
CORE = 1


def normed(x, gain):
    wide = x.astype(jnp.float32)
    scale = lax.rsqrt(jnp.mean(wide * wide, -1, keepdims=True) + 1e-6)
    return (wide * scale * gain.astype(jnp.float32)).astype(jnp.bfloat16)


def tables(rows):
    half = HEAD // 2
    angle = jnp.arange(rows).astype(jnp.float32)[:, None] * THETA ** (-jnp.arange(half, dtype=jnp.float32) / half)
    cos, sin = jnp.cos(angle), jnp.sin(angle)
    return jnp.concatenate([cos, cos], -1), jnp.concatenate([-sin, sin], -1)


def _dot(a, b, ca, cb):
    return lax.dot_general(a, b, (((ca,), (cb,)), ((), ())), preferred_element_type=jnp.float32)


def _qkv(block_ref, *refs, places, sizes, width, depth, slots, aliased):
    n = len(sizes)
    pieces, (wq, wk, wv, cos_ref, sin_ref) = refs[:n], refs[n : n + 5]
    out_ref, acc, low, held, w_sems, sems = refs[n + 5 + aliased :]
    k, steps = pl.program_id(0), pl.num_programs(0)

    def fetch(step):
        slot = lax.rem(step, slots)
        rows = pl.ds(pl.multiple_of(step * depth, depth), depth)
        return [pltpu.make_async_copy(w.at[rows, :], held.at[slot, :, pl.ds(i * width, width)], w_sems.at[slot, i])
                for i, w in enumerate((wq, wk, wv))]

    @pl.when(k == 0)
    def _():
        for step in range(slots - 1):
            for copy in fetch(step):
                copy.start()

    @pl.when(k + slots - 1 < steps)
    def _():
        for copy in fetch(k + slots - 1):
            copy.start()

    for copy in fetch(k):
        copy.wait()
    x = jnp.concatenate([p[...] for p in pieces], axis=0) if n > 1 else pieces[0][...]
    part = _dot(x, held[lax.rem(k, slots)], 1, 0)

    @pl.when(k == 0)
    def _():
        acc[...] = part

    @pl.when(k > 0)
    def _():
        acc[...] += part

    @pl.when(k == steps - 1)
    def _():
        copies, top = [], 0
        for i, ((block, size, row), rows) in enumerate(zip(places, sizes)):
            at = pl.multiple_of(block_ref[block] * size + row, 16)
            cos, sin = cos_ref[pl.ds(at, rows), :], sin_ref[pl.ds(at, rows), :]
            for c in range(0, 2 * width, HEAD):
                t = acc[top : top + rows, c : c + HEAD].astype(jnp.bfloat16).astype(jnp.float32)
                low[top : top + rows, c : c + HEAD] = (t * cos + pltpu.roll(t, HEAD // 2, 1) * sin).astype(jnp.bfloat16)
            low[top : top + rows, 2 * width :] = acc[top : top + rows, 2 * width :].astype(jnp.bfloat16)
            copies.append(pltpu.make_async_copy(low.at[pl.ds(top, rows), :], out_ref.at[pl.ds(at, rows), :], sems.at[i]))
            copies[-1].start()
            top += rows
        for copy in copies:
            copy.wait()


def qkv_of(pieces, places, blocks, wq, wk, wv, cos, sin, before=None):
    d, width = wq.shape
    total = cos.shape[0]
    sizes = tuple(p.shape[0] for p in pieces)
    m = sum(sizes)
    depth, slots = (1024, 3) if m <= 256 else (2048, 2)
    table = pl.BlockSpec((total, HEAD), lambda k, _: (0, 0))
    specs = [pl.BlockSpec((r, depth), lambda k, _: (0, k)) for r in sizes] + [pl.BlockSpec(memory_space=pl.ANY)] * 3 + [table] * 2
    given = [*pieces, wq, wk, wv, cos, sin]
    alias = {}
    if before is not None:
        alias = {1 + len(given): 0}
        given.append(before)
        specs.append(pl.BlockSpec(memory_space=pl.ANY))
    return pl.pallas_call(
        functools.partial(_qkv, places=places, sizes=sizes, width=width, depth=depth, slots=slots, aliased=int(before is not None)),
        grid_spec=pltpu.PrefetchScalarGridSpec(
            num_scalar_prefetch=1,
            grid=(d // depth,),
            in_specs=specs,
            out_specs=pl.BlockSpec(memory_space=pl.ANY),
            scratch_shapes=[pltpu.VMEM((m, 3 * width), jnp.float32), pltpu.VMEM((m, 3 * width), jnp.bfloat16),
                            pltpu.VMEM((slots, depth, 3 * width), jnp.bfloat16), pltpu.SemaphoreType.DMA((slots, 3)),
                            pltpu.SemaphoreType.DMA((len(sizes),))],
        ),
        out_shape=jax.ShapeDtypeStruct((total, 3 * width), jnp.bfloat16),
        input_output_aliases=alias,
        compiler_params=pltpu.CompilerParams(dimension_semantics=("arbitrary",), vmem_limit_bytes=VMEM),
        cost_estimate=pl.CostEstimate(flops=2 * m * d * 3 * width, transcendentals=0, bytes_accessed=2 * d * (m + 3 * width)),
        name="qkv",
    )(blocks, *given)


def _attend(block_ref, q_ref, k_ref, v_ref, o_ref, top_s, mix_s, gap_s, *, scale, bq, bk, heads, pick):
    low = k_ref.dtype
    iq = pick(pl.program_id(0), block_ref)
    e = scale * LOG2E

    gap_s[...] = lax.broadcasted_iota(jnp.int32, (bk, bq), 1) - lax.broadcasted_iota(jnp.int32, (bk, bq), 0)
    top_s[...] = jnp.full(top_s.shape, NEG, jnp.float32)
    mix_s[...] = jnp.zeros(mix_s.shape, jnp.float32)
    ones = jnp.ones((8, bk), low)

    def block(j, masked):
        here = pl.ds(pl.multiple_of(j * bk, bk), bk)
        cols = [slice(i * HEAD, (i + 1) * HEAD) for i in range(heads)]
        scores = [_dot(k_ref[here, c], q_ref[:, c], 1, 1) for c in cols]
        ok = gap_s[...] >= j * bk - iq * bq if masked else None
        weights, keeps = [], []
        for i, s in enumerate(scores):
            if masked:
                s = jnp.where(ok, s, HIDDEN)
            old = top_s[i : i + 1, :]
            top = jnp.maximum(old, s.max(axis=0, keepdims=True))
            top_s[i : i + 1, :] = top
            weights.append(jnp.exp2((s - top) * e).astype(low))
            keeps.append(jnp.exp2((old - top) * e))
        for i, (p, keep) in enumerate(zip(weights, keeps)):
            values = jnp.concatenate([v_ref[here, cols[i]].T, ones], axis=0)
            mix_s[i] = mix_s[i] * keep + _dot(values, p, 1, 0)

    whole = lax.div(iq * bq, bk)
    last = lax.div(iq * bq + bq + bk - 1, bk)
    lax.fori_loop(0, whole, lambda j, _: block(j, False), None)
    lax.fori_loop(whole, last, lambda j, _: block(j, True), None)
    for i in range(heads):
        o_ref[:, i * HEAD : (i + 1) * HEAD] = (mix_s[i, :HEAD, :] * (1 / mix_s[i, HEAD : HEAD + 1, :])).T.astype(o_ref.dtype)


def attention(qkv, flips, blocks, bq, bk=512):
    rows, width = qkv.shape[0], qkv.shape[1] // 3
    heads, n = width // HEAD, len(flips)

    def pick(i, block_ref):
        at = block_ref[flips[0]]
        for j in range(1, n):
            at = jnp.where(i == j, block_ref[flips[j]], at)
        return at >> 1

    return pl.pallas_call(
        functools.partial(_attend, scale=HEAD**-0.5, bq=bq, bk=bk, heads=heads, pick=pick),
        grid_spec=pltpu.PrefetchScalarGridSpec(
            num_scalar_prefetch=1,
            grid=(n,),
            in_specs=[pl.BlockSpec((bq, width), lambda i, b: (pick(i, b), 0)), pl.BlockSpec((rows, width), lambda i, b: (0, 1)),
                      pl.BlockSpec((rows, width), lambda i, b: (0, 2))],
            out_specs=pl.BlockSpec((bq, width), lambda i, b: (i, 0)),
            scratch_shapes=[pltpu.VMEM((heads, bq), jnp.float32), pltpu.VMEM((heads, HEAD + 8, bq), jnp.float32), pltpu.VMEM((bk, bq), jnp.int32)],
        ),
        out_shape=jax.ShapeDtypeStruct((n * bq, width), jnp.bfloat16),
        compiler_params=pltpu.CompilerParams(dimension_semantics=("arbitrary",), vmem_limit_bytes=VMEM),
        cost_estimate=pl.CostEstimate(flops=2 * n * bq * rows * width, transcendentals=heads * n * bq * rows // 2, bytes_accessed=8 * rows * width),
        name="attention",
    )(blocks, qkv, qkv, qkv)


def _project(block_ref, *refs, n, adds, outs, start, tile):
    seen, (wa, wb), refs = refs[: 2 * n], refs[2 * n : 2 * n + 2], refs[2 * n + 2 :]
    rows = seen[0].shape[0]
    join = lambda refs: jnp.concatenate([r[...] for r in refs], axis=0) if n > 1 else refs[0][...]
    term = _dot(join(seen[:n]), wa[...], 1, 0) + _dot(join(seen[n:]), wb[...], 1, 0)
    column = (start + pl.program_id(0)) * tile
    inside = lambda low, high: (column >= low) & (column < high)
    for (i, low, high, whole), out in zip(outs, refs[len(adds) :]):

        def write(i=i, out=out):
            total = term[i * rows : (i + 1) * rows]
            for (owner, low, high, whole), ref in zip(adds, refs):
                if owner == i:
                    t = ref[...].astype(jnp.float32)
                    total = total + (t if whole else jnp.where(inside(low, high), t, 0.0))
            out[...] = total.astype(out.dtype)

        if whole:
            write()
        else:
            pl.when(inside(low, high))(write)


def project(found, weights, blocks, adds, outs, first, columns, rows=128, tile=TILE):
    n, width = len(found), found[0][0].shape[1]
    start = first // tile
    mine = lambda at: pl.BlockSpec((rows, width), lambda j, b, at=at: (2 * at + (b[0] & 1), 0))
    span = lambda low, high: pl.BlockSpec((rows, tile), lambda j, b: (0, jnp.clip(start + j - low // tile, 0, (high - low) // tile - 1)))
    specs = [mine(at) for _ in range(2) for _, _, at in found]
    specs += [pl.BlockSpec((width, tile), lambda j, b: (0, start + j))] * 2
    adds = [a for a in adds if a[1] < first + columns and first < a[2]]
    whole = lambda low, high: low <= first and first + columns <= high
    return pl.pallas_call(
        functools.partial(_project, n=n, adds=tuple((i, low, high, whole(low, high)) for i, low, high, _ in adds),
                          outs=tuple((i, low, high, whole(low, high)) for i, low, high, _ in outs), start=start, tile=tile),
        grid_spec=pltpu.PrefetchScalarGridSpec(
            num_scalar_prefetch=1,
            grid=(columns // tile,),
            in_specs=specs + [span(low, high) for _, low, high, _ in adds],
            out_specs=[span(low, high) for _, low, high, _ in outs],
        ),
        out_shape=[jax.ShapeDtypeStruct((rows, high - low), kind) for _, low, high, kind in outs],
        compiler_params=pltpu.CompilerParams(dimension_semantics=("arbitrary",), vmem_limit_bytes=VMEM),
        cost_estimate=pl.CostEstimate(flops=4 * n * rows * width * columns, transcendentals=0,
                                      bytes_accessed=4 * width * columns + 4 * n * rows * (width + columns)),
        name="project",
    )(blocks, *[f[0] for f in found], *[f[1] for f in found], *weights, *[a[3] for a in adds])


def _sum(*refs, n):
    total = refs[0][...]
    for ref in refs[1:n]:
        total = total + ref[...].astype(jnp.float32)
    refs[-1][...] = total.astype(refs[-1].dtype)


def finish(terms, first, columns, before=None, tile=1024):
    rows, here = terms[0].shape
    start = first // tile
    given, specs, alias = list(terms), [pl.BlockSpec((rows, tile), lambda j: (0, j))] * len(terms), {}
    if before is not None:
        alias = {len(given): 0}
        given.append(before)
        specs.append(pl.BlockSpec(memory_space=pl.ANY))
    return pl.pallas_call(
        functools.partial(_sum, n=len(terms)),
        grid=(here // tile,),
        in_specs=specs,
        out_specs=pl.BlockSpec((rows, tile), lambda j: (0, start + j)),
        out_shape=jax.ShapeDtypeStruct((rows, columns), jnp.bfloat16),
        input_output_aliases=alias,
        compiler_params=pltpu.CompilerParams(dimension_semantics=("arbitrary",), vmem_limit_bytes=VMEM),
        cost_estimate=pl.CostEstimate(flops=rows * here * len(terms), transcendentals=0, bytes_accessed=12 * rows * here),
        name="finish",
    )(*given)


def solution(mesh):
    devices = mesh.shape["tp"]

    def hop(t, flip):
        pairs = [(i, i ^ flip) for i in range(devices)]
        return lax.ppermute(t, "tp", pairs)

    def step(x, gain, wq, wk, wv, wo):
        return body(x, gain, wq, wk, wv, wo)

    def body(x, gain, wq, wk, wv, wo):
        me = lax.axis_index("tp").astype(jnp.int32)
        rows, d = x.shape
        total = rows * devices
        third = d // 3
        half = rows // 2
        pair = [LINKS[l] | LINKS[l - 1] for l in range(3)]
        a = normed(x, gain)
        cos, sin = tables(total)
        tie = lax.optimization_barrier
        blocks = me ^ jnp.arange(devices, dtype=jnp.int32)

        near = [[hop(a[h * half : (h + 1) * half], LINKS[l]) for l in range(3)] for h in range(2)]
        other = hop(a, CORE)

        def stage(found, before):
            places = tuple((flip, rows, row) for _, flip, row in found)
            return qkv_of([t for t, _, _ in found], places, blocks, wq, wk, wv, cos, sin, before)

        def own(ts, flips, row):
            return [(t, flip, row) for t, flip in zip(ts, flips)]

        def theirs(ts, flips, row):
            return [(hop(t, CORE), flip ^ CORE, row) for t, flip in zip(ts, flips)]

        def farthest(h):
            return [(hop(mid[h][(h + 2) % 3], LINKS[h]), FAR, h * half)]

        qkv = stage([(a, 0, 0), (other, CORE, 0)], None)
        near[0], qkv = tie((near[0], qkv))
        mid = [[hop(near[0][l - 1], LINKS[l]) for l in range(3)], None]
        late = theirs(near[0], LINKS, 0)
        qkv = stage(own(near[0], LINKS, 0), qkv)
        near[1], qkv = tie((near[1], qkv))
        mid[1] = [hop(near[1][l - 1], LINKS[l]) for l in range(3)]
        now, late = late + own(near[1], LINKS, half), theirs(near[1], LINKS, half)
        qkv = stage(now, qkv)
        mid[0], qkv, wo_in = tie((mid[0], qkv, wo))
        far = farthest(0)
        now, late = late + own(mid[0], pair, 0), theirs(mid[0], pair, 0)
        qkv = stage(now, qkv)
        mid[1], qkv = tie((mid[1], qkv))
        wo_other = hop(wo_in, CORE)
        far += farthest(1)
        now, late = late + own(mid[1], pair, half), theirs(mid[1], pair, half)
        qkv = stage(now, qkv)
        qkv = stage(late + far + [(hop(t, CORE), FAR ^ CORE, row) for t, _, row in far], qkv)

        weights = (wo, wo_other)

        def attended(flips):
            t = attention(qkv, flips, blocks, 2 * rows)
            other = hop(t, CORE)
            return {flip: (t, other, i) for i, flip in enumerate(flips)}

        seen = attended((FAR,))

        low, wide = jnp.bfloat16, jnp.float32
        cols = [(h * d // 2, (h + 1) * d // 2) for h in range(2)]
        out = project([seen[FAR]], weights, blocks, [], [(0, l * third, (l + 1) * third, low) for l in range(3)], 0, d)
        far_in = [hop(out[l], LINKS[l]) for l in range(3)]
        qkv, out = tie((qkv, out))
        seen |= attended(tuple(pair))
        mid_in, out = [], None
        for lo, hi in cols:
            adds = [(l, (l + 1) % 3 * third, ((l + 1) % 3 + 1) * third, far_in[(l + 1) % 3]) for l in range(3)]
            out = project([seen[f] for f in pair], weights, blocks, adds, [(l, lo, hi, low) for l in range(3)], lo, hi - lo)
            mid_in.append([hop(out[l], LINKS[l]) for l in range(3)])
        qkv, out = tie((qkv, out))
        seen |= attended((*LINKS, 0))
        rest, near_in = [], []
        for h, (lo, hi) in enumerate(cols):
            adds = [(l, lo, hi, mid_in[h][(l + 1) % 3]) for l in range(3)] + [(3, 0, d, x)]
            out = project([seen[f] for f in (*LINKS, 0)], weights, blocks, adds, [(l, lo, hi, low if l < 3 else wide) for l in range(4)], lo, hi - lo)
            near_in.append([hop(out[l], LINKS[l]) for l in range(3)])
            rest.append(out[3])
        y = None
        for h, (lo, hi) in enumerate(cols):
            y = finish([rest[h], *near_in[h]], lo, d, y)
        return y

    tokens, columns = P(("dp", "tp"), None), P(None, "tp")
    step = jax.shard_map(
        step,
        mesh=mesh,
        in_specs=(tokens, P(None), columns, columns, columns, P("tp", None)),
        out_specs=tokens,
        check_vma=False,
    )
    return step
```

```python
import functools

import jax
import jax.numpy as jnp
from jax import lax
from jax.experimental import pallas as pl
from jax.experimental.pallas import tpu as pltpu
from jax.sharding import PartitionSpec as P


NEG = -1e30
HIDDEN = 2 * NEG
LOG2E = 1.4426950408889634
VMEM = 63 * 2**20
TILE = 2048
HEAD = 128
THETA = 10000
LINKS = (8, 4, 2)
FAR = 14
CORE = 1


def normed(x, gain):
    wide = x.astype(jnp.float32)
    scale = lax.rsqrt(jnp.mean(wide * wide, -1, keepdims=True) + 1e-6)
    return (wide * scale * gain.astype(jnp.float32)).astype(jnp.bfloat16)


def tables(rows):
    half = HEAD // 2
    angle = jnp.arange(rows).astype(jnp.float32)[:, None] * THETA ** (-jnp.arange(half, dtype=jnp.float32) / half)
    cos, sin = jnp.cos(angle), jnp.sin(angle)
    return jnp.concatenate([cos, cos], -1), jnp.concatenate([-sin, sin], -1)


def _dot(a, b, ca, cb):
    return lax.dot_general(a, b, (((ca,), (cb,)), ((), ())), preferred_element_type=jnp.float32)


def _qkv(block_ref, *refs, places, sizes, width, depth, slots, aliased):
    n = len(sizes)
    pieces, (wq, wk, wv, cos_ref, sin_ref) = refs[:n], refs[n : n + 5]
    out_ref, acc, low, held, w_sems, sems = refs[n + 5 + aliased :]
    k, steps = pl.program_id(0), pl.num_programs(0)

    def fetch(step):
        slot = lax.rem(step, slots)
        rows = pl.ds(pl.multiple_of(step * depth, depth), depth)
        return [pltpu.make_async_copy(w.at[rows, :], held.at[slot, :, pl.ds(i * width, width)], w_sems.at[slot, i])
                for i, w in enumerate((wq, wk, wv))]

    @pl.when(k == 0)
    def _():
        for step in range(slots - 1):
            for copy in fetch(step):
                copy.start()
        acc[...] = jnp.zeros_like(acc)

    @pl.when(k + slots - 1 < steps)
    def _():
        for copy in fetch(k + slots - 1):
            copy.start()

    for copy in fetch(k):
        copy.wait()
    x = jnp.concatenate([p[...] for p in pieces], axis=0) if n > 1 else pieces[0][...]
    acc[...] += _dot(x, held[lax.rem(k, slots)], 1, 0)

    @pl.when(k == steps - 1)
    def _():
        copies, top = [], 0
        for i, ((block, size, row), rows) in enumerate(zip(places, sizes)):
            at = pl.multiple_of(block_ref[block] * size + row, 16)
            cos, sin = cos_ref[pl.ds(at, rows), :], sin_ref[pl.ds(at, rows), :]
            for c in range(0, 2 * width, HEAD):
                t = acc[top : top + rows, c : c + HEAD].astype(jnp.bfloat16).astype(jnp.float32)
                low[top : top + rows, c : c + HEAD] = (t * cos + pltpu.roll(t, HEAD // 2, 1) * sin).astype(jnp.bfloat16)
            low[top : top + rows, 2 * width :] = acc[top : top + rows, 2 * width :].astype(jnp.bfloat16)
            copies.append(pltpu.make_async_copy(low.at[pl.ds(top, rows), :], out_ref.at[pl.ds(at, rows), :], sems.at[i]))
            copies[-1].start()
            top += rows
        for copy in copies:
            copy.wait()


def qkv_of(pieces, places, blocks, wq, wk, wv, cos, sin, before=None):
    d, width = wq.shape
    total = cos.shape[0]
    sizes = tuple(p.shape[0] for p in pieces)
    m = sum(sizes)
    depth, slots = (1024, 3) if m <= 256 else (2048, 2)
    table = pl.BlockSpec((total, HEAD), lambda k, _: (0, 0))
    specs = [pl.BlockSpec((r, depth), lambda k, _: (0, k)) for r in sizes] + [pl.BlockSpec(memory_space=pl.ANY)] * 3 + [table] * 2
    given = [*pieces, wq, wk, wv, cos, sin]
    alias = {}
    if before is not None:
        alias = {1 + len(given): 0}
        given.append(before)
        specs.append(pl.BlockSpec(memory_space=pl.ANY))
    return pl.pallas_call(
        functools.partial(_qkv, places=places, sizes=sizes, width=width, depth=depth, slots=slots, aliased=int(before is not None)),
        grid_spec=pltpu.PrefetchScalarGridSpec(
            num_scalar_prefetch=1,
            grid=(d // depth,),
            in_specs=specs,
            out_specs=pl.BlockSpec(memory_space=pl.ANY),
            scratch_shapes=[pltpu.VMEM((m, 3 * width), jnp.float32), pltpu.VMEM((m, 3 * width), jnp.bfloat16),
                            pltpu.VMEM((slots, depth, 3 * width), jnp.bfloat16), pltpu.SemaphoreType.DMA((slots, 3)),
                            pltpu.SemaphoreType.DMA((len(sizes),))],
        ),
        out_shape=jax.ShapeDtypeStruct((total, 3 * width), jnp.bfloat16),
        input_output_aliases=alias,
        compiler_params=pltpu.CompilerParams(dimension_semantics=("arbitrary",), vmem_limit_bytes=VMEM),
        cost_estimate=pl.CostEstimate(flops=2 * m * d * 3 * width, transcendentals=0, bytes_accessed=2 * d * (m + 3 * width)),
        name="qkv",
    )(blocks, *given)


def _attend(block_ref, q_ref, k_ref, v_ref, o_ref, top_s, mix_s, gap_s, *, scale, bq, bk, heads, pick):
    low = k_ref.dtype
    iq = pick(pl.program_id(0), block_ref)
    e = scale * LOG2E

    gap_s[...] = lax.broadcasted_iota(jnp.int32, (bk, bq), 1) - lax.broadcasted_iota(jnp.int32, (bk, bq), 0)
    top_s[...] = jnp.full(top_s.shape, NEG, jnp.float32)
    mix_s[...] = jnp.zeros(mix_s.shape, jnp.float32)
    ones = jnp.ones((8, bk), low)

    def block(j, masked):
        here = pl.ds(pl.multiple_of(j * bk, bk), bk)
        cols = [slice(i * HEAD, (i + 1) * HEAD) for i in range(heads)]
        scores = [_dot(k_ref[here, c], q_ref[:, c], 1, 1) for c in cols]
        ok = gap_s[...] >= j * bk - iq * bq if masked else None
        weights, keeps = [], []
        for i, s in enumerate(scores):
            if masked:
                s = jnp.where(ok, s, HIDDEN)
            old = top_s[i : i + 1, :]
            top = jnp.maximum(old, s.max(axis=0, keepdims=True))
            top_s[i : i + 1, :] = top
            weights.append(jnp.exp2((s - top) * e).astype(low))
            keeps.append(jnp.exp2((old - top) * e))
        for i, (p, keep) in enumerate(zip(weights, keeps)):
            values = jnp.concatenate([v_ref[here, cols[i]].T, ones], axis=0)
            mix_s[i] = mix_s[i] * keep + _dot(values, p, 1, 0)

    whole = lax.div(iq * bq, bk)
    last = lax.div(iq * bq + bq + bk - 1, bk)
    lax.fori_loop(0, whole, lambda j, _: block(j, False), None)
    lax.fori_loop(whole, last, lambda j, _: block(j, True), None)
    for i in range(heads):
        o_ref[:, i * HEAD : (i + 1) * HEAD] = (mix_s[i, :HEAD, :] * (1 / mix_s[i, HEAD : HEAD + 1, :])).T.astype(o_ref.dtype)


def attention(qkv, flips, blocks, bq, bk=512):
    rows, width = qkv.shape[0], qkv.shape[1] // 3
    heads, n = width // HEAD, len(flips)

    def pick(i, block_ref):
        at = block_ref[flips[0]]
        for j in range(1, n):
            at = jnp.where(i == j, block_ref[flips[j]], at)
        return at >> 1

    return pl.pallas_call(
        functools.partial(_attend, scale=HEAD**-0.5, bq=bq, bk=bk, heads=heads, pick=pick),
        grid_spec=pltpu.PrefetchScalarGridSpec(
            num_scalar_prefetch=1,
            grid=(n,),
            in_specs=[pl.BlockSpec((bq, width), lambda i, b: (pick(i, b), 0)), pl.BlockSpec((rows, width), lambda i, b: (0, 1)),
                      pl.BlockSpec((rows, width), lambda i, b: (0, 2))],
            out_specs=pl.BlockSpec((bq, width), lambda i, b: (i, 0)),
            scratch_shapes=[pltpu.VMEM((heads, bq), jnp.float32), pltpu.VMEM((heads, HEAD + 8, bq), jnp.float32), pltpu.VMEM((bk, bq), jnp.int32)],
        ),
        out_shape=jax.ShapeDtypeStruct((n * bq, width), jnp.bfloat16),
        compiler_params=pltpu.CompilerParams(dimension_semantics=("arbitrary",), vmem_limit_bytes=VMEM),
        cost_estimate=pl.CostEstimate(flops=2 * n * bq * rows * width, transcendentals=heads * n * bq * rows // 2, bytes_accessed=8 * rows * width),
        name="attention",
    )(blocks, qkv, qkv, qkv)


def _project(block_ref, *refs, n, adds, outs, start, tile):
    seen, (wa, wb), refs = refs[: 2 * n], refs[2 * n : 2 * n + 2], refs[2 * n + 2 :]
    rows = seen[0].shape[0]
    join = lambda refs: jnp.concatenate([r[...] for r in refs], axis=0) if n > 1 else refs[0][...]
    term = _dot(join(seen[:n]), wa[...], 1, 0) + _dot(join(seen[n:]), wb[...], 1, 0)
    column = (start + pl.program_id(0)) * tile
    inside = lambda low, high: (column >= low) & (column < high)
    for (i, low, high, whole), out in zip(outs, refs[len(adds) :]):

        def write(i=i, out=out):
            total = term[i * rows : (i + 1) * rows]
            for (owner, low, high, whole), ref in zip(adds, refs):
                if owner == i:
                    t = ref[...].astype(jnp.float32)
                    total = total + (t if whole else jnp.where(inside(low, high), t, 0.0))
            out[...] = total.astype(out.dtype)

        if whole:
            write()
        else:
            pl.when(inside(low, high))(write)


def project(found, weights, blocks, adds, outs, first, columns, rows=128, tile=TILE):
    n, width = len(found), found[0][0].shape[1]
    start = first // tile
    mine = lambda at: pl.BlockSpec((rows, width), lambda j, b, at=at: (2 * at + (b[0] & 1), 0))
    span = lambda low, high: pl.BlockSpec((rows, tile), lambda j, b: (0, jnp.clip(start + j - low // tile, 0, (high - low) // tile - 1)))
    specs = [mine(at) for _ in range(2) for _, _, at in found]
    specs += [pl.BlockSpec((width, tile), lambda j, b: (0, start + j))] * 2
    adds = [a for a in adds if a[1] < first + columns and first < a[2]]
    whole = lambda low, high: low <= first and first + columns <= high
    return pl.pallas_call(
        functools.partial(_project, n=n, adds=tuple((i, low, high, whole(low, high)) for i, low, high, _ in adds),
                          outs=tuple((i, low, high, whole(low, high)) for i, low, high, _ in outs), start=start, tile=tile),
        grid_spec=pltpu.PrefetchScalarGridSpec(
            num_scalar_prefetch=1,
            grid=(columns // tile,),
            in_specs=specs + [span(low, high) for _, low, high, _ in adds],
            out_specs=[span(low, high) for _, low, high, _ in outs],
        ),
        out_shape=[jax.ShapeDtypeStruct((rows, high - low), kind) for _, low, high, kind in outs],
        compiler_params=pltpu.CompilerParams(dimension_semantics=("arbitrary",), vmem_limit_bytes=VMEM),
        cost_estimate=pl.CostEstimate(flops=4 * n * rows * width * columns, transcendentals=0,
                                      bytes_accessed=4 * width * columns + 4 * n * rows * (width + columns)),
        name="project",
    )(blocks, *[f[0] for f in found], *[f[1] for f in found], *weights, *[a[3] for a in adds])


def _sum(*refs, n):
    total = refs[0][...]
    for ref in refs[1:n]:
        total = total + ref[...].astype(jnp.float32)
    refs[-1][...] = total.astype(refs[-1].dtype)


def finish(terms, first, columns, before=None, tile=2048):
    rows, here = terms[0].shape
    start = first // tile
    given, specs, alias = list(terms), [pl.BlockSpec((rows, tile), lambda j: (0, j))] * len(terms), {}
    if before is not None:
        alias = {len(given): 0}
        given.append(before)
        specs.append(pl.BlockSpec(memory_space=pl.ANY))
    return pl.pallas_call(
        functools.partial(_sum, n=len(terms)),
        grid=(here // tile,),
        in_specs=specs,
        out_specs=pl.BlockSpec((rows, tile), lambda j: (0, start + j)),
        out_shape=jax.ShapeDtypeStruct((rows, columns), jnp.bfloat16),
        input_output_aliases=alias,
        compiler_params=pltpu.CompilerParams(dimension_semantics=("arbitrary",), vmem_limit_bytes=VMEM),
        cost_estimate=pl.CostEstimate(flops=rows * here * len(terms), transcendentals=0, bytes_accessed=12 * rows * here),
        name="finish",
    )(*given)


def solution(mesh):
    devices = mesh.shape["tp"]

    def hop(t, flip):
        pairs = [(i, i ^ flip) for i in range(devices)]
        return lax.ppermute(t, "tp", pairs)

    def step(x, gain, wq, wk, wv, wo):
        return body(x, gain, wq, wk, wv, wo)

    def body(x, gain, wq, wk, wv, wo):
        me = lax.axis_index("tp").astype(jnp.int32)
        rows, d = x.shape
        total = rows * devices
        third = d // 3
        half = rows // 2
        pair = [LINKS[l] | LINKS[l - 1] for l in range(3)]
        a = [normed(x[h * half : (h + 1) * half], gain) for h in range(2)]
        cos, sin = tables(total)
        tie = lax.optimization_barrier
        blocks = me ^ jnp.arange(devices, dtype=jnp.int32)

        near = [[hop(a[h], LINKS[l]) for l in range(3)] for h in range(2)]
        other = [hop(t, CORE) for t in a]

        def stage(found, before):
            places = tuple((flip, rows, row) for _, flip, row in found)
            return qkv_of([t for t, _, _ in found], places, blocks, wq, wk, wv, cos, sin, before)

        def own(ts, flips, row):
            return [(t, flip, row) for t, flip in zip(ts, flips)]

        def theirs(ts, flips, row):
            return [(hop(t, CORE), flip ^ CORE, row) for t, flip in zip(ts, flips)]

        def farthest(h):
            return [(hop(mid[h][(h + 2) % 3], LINKS[h]), FAR, h * half)]

        qkv = stage([(t, flip, h * half) for ts, flip in ((a, 0), (other, CORE)) for h, t in enumerate(ts)], None)
        near[0], qkv = tie((near[0], qkv))
        mid = [[hop(near[0][l - 1], LINKS[l]) for l in range(3)], None]
        late = theirs(near[0], LINKS, 0)
        qkv = stage(own(near[0], LINKS, 0), qkv)
        near[1], qkv = tie((near[1], qkv))
        mid[1] = [hop(near[1][l - 1], LINKS[l]) for l in range(3)]
        now, late = late + own(near[1], LINKS, half), theirs(near[1], LINKS, half)
        qkv = stage(now, qkv)
        mid[0], qkv, wo_in = tie((mid[0], qkv, wo))
        far = farthest(0)
        now, late = late + own(mid[0], pair, 0), theirs(mid[0], pair, 0)
        qkv = stage(now, qkv)
        mid[1], qkv = tie((mid[1], qkv))
        wo_other = hop(wo_in, CORE)
        far += farthest(1)
        now, late = late + own(mid[1], pair, half), theirs(mid[1], pair, half)
        qkv = stage(now, qkv)
        qkv = stage(late + far + [(hop(t, CORE), FAR ^ CORE, row) for t, _, row in far], qkv)

        weights = (wo, wo_other)

        def attended(flips):
            t = attention(qkv, flips, blocks, 2 * rows)
            other = hop(t, CORE)
            return {flip: (t, other, i) for i, flip in enumerate(flips)}

        seen = attended((FAR,))

        low, wide = jnp.bfloat16, jnp.float32
        thirds = [(l * third, (l + 1) * third) for l in range(3)]
        out = project([seen[FAR]], weights, blocks, [], [(0, *thirds[0], low)], 0, third)
        far_in = [hop(out[0], LINKS[0])]
        out = project([seen[FAR]], weights, blocks, [], [(0, *thirds[l], low) for l in (1, 2)], third, 2 * third)
        far_in += [hop(t, LINKS[l]) for l, t in zip((1, 2), out)]
        qkv, out = tie((qkv, out))
        seen |= attended(tuple(pair))
        mid_in, out = [], None
        for lo, hi in ((0, third), (third, d)):
            adds = [(l, (l + 1) % 3 * third, ((l + 1) % 3 + 1) * third, far_in[(l + 1) % 3]) for l in range(3)]
            out = project([seen[f] for f in pair], weights, blocks, adds, [(l, lo, hi, low) for l in range(3)], lo, hi - lo)
            mid_in.append([(lo, hi, hop(out[l], LINKS[l])) for l in range(3)])
        qkv, out = tie((qkv, out))
        seen |= attended((*LINKS, 0))
        rest, near_in = [], []
        for h, (lo, hi) in enumerate(thirds):
            adds = [(l, *mid_in[min(h, 1)][(l + 1) % 3]) for l in range(3)] + [(3, 0, d, x)]
            out = project([seen[f] for f in (*LINKS, 0)], weights, blocks, adds, [(l, lo, hi, low if l < 3 else wide) for l in range(4)], lo, hi - lo)
            near_in.append([hop(out[l], LINKS[l]) for l in range(3)])
            rest.append(out[3])
        y = None
        for h, (lo, _) in enumerate(thirds):
            y = finish([rest[h], *near_in[h]], lo, d, y)
        return y

    tokens, columns = P(("dp", "tp"), None), P(None, "tp")
    step = jax.shard_map(
        step,
        mesh=mesh,
        in_specs=(tokens, P(None), columns, columns, columns, P("tp", None)),
        out_specs=tokens,
        check_vma=False,
    )
    return step
```

```python
import functools

import jax
import jax.numpy as jnp
from jax import lax
from jax.experimental import pallas as pl
from jax.experimental.pallas import tpu as pltpu
from jax.sharding import PartitionSpec as P


NEG = -1e30
HIDDEN = 2 * NEG
LOG2E = 1.4426950408889634
VMEM = 63 * 2**20
HEAD = 128
THETA = 10000
LINKS = (8, 4, 2)
FAR = 14
CORE = 1


def normed(x, gain):
    wide = x.astype(jnp.float32)
    scale = lax.rsqrt(jnp.mean(wide * wide, -1, keepdims=True) + 1e-6)
    return (wide * scale * gain.astype(jnp.float32)).astype(jnp.bfloat16)


def tables(rows):
    half = HEAD // 2
    angle = jnp.arange(rows).astype(jnp.float32)[:, None] * THETA ** (-jnp.arange(half, dtype=jnp.float32) / half)
    cos, sin = jnp.cos(angle), jnp.sin(angle)
    return jnp.concatenate([cos, cos], -1), jnp.concatenate([-sin, sin], -1)


def _dot(a, b, ca, cb):
    return lax.dot_general(a, b, (((ca,), (cb,)), ((), ())), preferred_element_type=jnp.float32)


def _qkv(block_ref, *refs, places, sizes, width, depth, slots, aliased):
    n = len(sizes)
    pieces, (wq, wk, wv, cos_ref, sin_ref) = refs[:n], refs[n : n + 5]
    out_ref, acc, low, held, w_sems, sems = refs[n + 5 + aliased :]
    k, steps = pl.program_id(0), pl.num_programs(0)

    def fetch(step):
        slot = lax.rem(step, slots)
        rows = pl.ds(pl.multiple_of(step * depth, depth), depth)
        return [pltpu.make_async_copy(w.at[rows, :], held.at[slot, :, pl.ds(i * width, width)], w_sems.at[slot, i])
                for i, w in enumerate((wq, wk, wv))]

    @pl.when(k == 0)
    def _():
        for step in range(slots - 1):
            for copy in fetch(step):
                copy.start()
        acc[...] = jnp.zeros_like(acc)

    @pl.when(k + slots - 1 < steps)
    def _():
        for copy in fetch(k + slots - 1):
            copy.start()

    for copy in fetch(k):
        copy.wait()
    x = jnp.concatenate([p[...] for p in pieces], axis=0) if n > 1 else pieces[0][...]
    acc[...] += _dot(x, held[lax.rem(k, slots)], 1, 0)

    @pl.when(k == steps - 1)
    def _():
        copies, top = [], 0
        for i, ((block, size, row), rows) in enumerate(zip(places, sizes)):
            at = pl.multiple_of(block_ref[block] * size + row, 16)
            cos, sin = cos_ref[pl.ds(at, rows), :], sin_ref[pl.ds(at, rows), :]
            for c in range(0, 2 * width, HEAD):
                t = acc[top : top + rows, c : c + HEAD].astype(jnp.bfloat16).astype(jnp.float32)
                low[top : top + rows, c : c + HEAD] = (t * cos + pltpu.roll(t, HEAD // 2, 1) * sin).astype(jnp.bfloat16)
            low[top : top + rows, 2 * width :] = acc[top : top + rows, 2 * width :].astype(jnp.bfloat16)
            copies.append(pltpu.make_async_copy(low.at[pl.ds(top, rows), :], out_ref.at[pl.ds(at, rows), :], sems.at[i]))
            copies[-1].start()
            top += rows
        for copy in copies:
            copy.wait()


def qkv_of(pieces, places, blocks, wq, wk, wv, cos, sin, before=None):
    d, width = wq.shape
    total = cos.shape[0]
    sizes = tuple(p.shape[0] for p in pieces)
    m = sum(sizes)
    depth, slots = (1024, 3) if m <= 384 else (2048, 2)
    table = pl.BlockSpec((total, HEAD), lambda k, _: (0, 0))
    specs = [pl.BlockSpec((r, depth), lambda k, _: (0, k)) for r in sizes] + [pl.BlockSpec(memory_space=pl.ANY)] * 3 + [table] * 2
    given = [*pieces, wq, wk, wv, cos, sin]
    alias = {}
    if before is not None:
        alias = {1 + len(given): 0}
        given.append(before)
        specs.append(pl.BlockSpec(memory_space=pl.ANY))
    return pl.pallas_call(
        functools.partial(_qkv, places=places, sizes=sizes, width=width, depth=depth, slots=slots, aliased=int(before is not None)),
        grid_spec=pltpu.PrefetchScalarGridSpec(
            num_scalar_prefetch=1,
            grid=(d // depth,),
            in_specs=specs,
            out_specs=pl.BlockSpec(memory_space=pl.ANY),
            scratch_shapes=[pltpu.VMEM((m, 3 * width), jnp.float32), pltpu.VMEM((m, 3 * width), jnp.bfloat16),
                            pltpu.VMEM((slots, depth, 3 * width), jnp.bfloat16), pltpu.SemaphoreType.DMA((slots, 3)),
                            pltpu.SemaphoreType.DMA((len(sizes),))],
        ),
        out_shape=jax.ShapeDtypeStruct((total, 3 * width), jnp.bfloat16),
        input_output_aliases=alias,
        compiler_params=pltpu.CompilerParams(dimension_semantics=("arbitrary",), vmem_limit_bytes=VMEM),
        cost_estimate=pl.CostEstimate(flops=2 * m * d * 3 * width, transcendentals=0, bytes_accessed=2 * d * (m + 3 * width)),
        name="qkv",
    )(blocks, *given)


def _attend(block_ref, q_ref, k_ref, v_ref, o_ref, top_s, mix_s, gap_s, *, scale, bq, bk, heads, pick):
    low = k_ref.dtype
    iq = pick(pl.program_id(0), block_ref)
    e = scale * LOG2E

    gap_s[...] = lax.broadcasted_iota(jnp.int32, (bk, bq), 1) - lax.broadcasted_iota(jnp.int32, (bk, bq), 0)
    top_s[...] = jnp.full(top_s.shape, NEG, jnp.float32)
    mix_s[...] = jnp.zeros(mix_s.shape, jnp.float32)
    ones = jnp.ones((8, bk), low)

    def block(j, masked):
        here = pl.ds(pl.multiple_of(j * bk, bk), bk)
        cols = [slice(i * HEAD, (i + 1) * HEAD) for i in range(heads)]
        scores = [_dot(k_ref[here, c], q_ref[:, c], 1, 1) for c in cols]
        ok = gap_s[...] >= j * bk - iq * bq if masked else None
        weights, keeps = [], []
        for i, s in enumerate(scores):
            if masked:
                s = jnp.where(ok, s, HIDDEN)
            old = top_s[i : i + 1, :]
            top = jnp.maximum(old, s.max(axis=0, keepdims=True))
            top_s[i : i + 1, :] = top
            weights.append(jnp.exp2((s - top) * e).astype(low))
            keeps.append(jnp.exp2((old - top) * e))
        for i, (p, keep) in enumerate(zip(weights, keeps)):
            values = jnp.concatenate([v_ref[here, cols[i]].T, ones], axis=0)
            mix_s[i] = mix_s[i] * keep + _dot(values, p, 1, 0)

    whole = lax.div(iq * bq, bk)
    last = lax.div(iq * bq + bq + bk - 1, bk)
    lax.fori_loop(0, whole, lambda j, _: block(j, False), None)
    lax.fori_loop(whole, last, lambda j, _: block(j, True), None)
    for i in range(heads):
        o_ref[:, i * HEAD : (i + 1) * HEAD] = (mix_s[i, :HEAD, :] * (1 / mix_s[i, HEAD : HEAD + 1, :])).T.astype(o_ref.dtype)


def attention(qkv, flips, blocks, bq, bk=512):
    rows, width = qkv.shape[0], qkv.shape[1] // 3
    heads, n = width // HEAD, len(flips)

    def pick(i, block_ref):
        at = block_ref[flips[0]]
        for j in range(1, n):
            at = jnp.where(i == j, block_ref[flips[j]], at)
        return at >> 1

    return pl.pallas_call(
        functools.partial(_attend, scale=HEAD**-0.5, bq=bq, bk=bk, heads=heads, pick=pick),
        grid_spec=pltpu.PrefetchScalarGridSpec(
            num_scalar_prefetch=1,
            grid=(n,),
            in_specs=[pl.BlockSpec((bq, width), lambda i, b: (pick(i, b), 0)), pl.BlockSpec((rows, width), lambda i, b: (0, 1)),
                      pl.BlockSpec((rows, width), lambda i, b: (0, 2))],
            out_specs=pl.BlockSpec((bq, width), lambda i, b: (i, 0)),
            scratch_shapes=[pltpu.VMEM((heads, bq), jnp.float32), pltpu.VMEM((heads, HEAD + 8, bq), jnp.float32), pltpu.VMEM((bk, bq), jnp.int32)],
        ),
        out_shape=jax.ShapeDtypeStruct((n * bq, width), jnp.bfloat16),
        compiler_params=pltpu.CompilerParams(dimension_semantics=("arbitrary",), vmem_limit_bytes=VMEM),
        cost_estimate=pl.CostEstimate(flops=2 * n * bq * rows * width, transcendentals=heads * n * bq * rows // 2, bytes_accessed=8 * rows * width),
        name="attention",
    )(blocks, qkv, qkv, qkv)


def _project(block_ref, *refs, n, adds, outs, start, tile):
    seen, (wa, wb), refs = refs[: 2 * n], refs[2 * n : 2 * n + 2], refs[2 * n + 2 :]
    rows = seen[0].shape[0]
    join = lambda refs: jnp.concatenate([r[...] for r in refs], axis=0) if n > 1 else refs[0][...]
    term = _dot(join(seen[:n]), wa[...], 1, 0) + _dot(join(seen[n:]), wb[...], 1, 0)
    column = (start + pl.program_id(0)) * tile
    inside = lambda low, high: (column >= low) & (column < high)
    for (i, low, high, whole), out in zip(outs, refs[len(adds) :]):

        def write(i=i, out=out):
            total = term[i * rows : (i + 1) * rows]
            for (owner, low, high, whole), ref in zip(adds, refs):
                if owner == i:
                    t = ref[...].astype(jnp.float32)
                    total = total + (t if whole else jnp.where(inside(low, high), t, 0.0))
            out[...] = total.astype(out.dtype)

        if whole:
            write()
        else:
            pl.when(inside(low, high))(write)


def project(found, weights, blocks, adds, outs, first, columns, rows=128):
    n, width = len(found), found[0][0].shape[1]
    tile = 1024 if n * columns > 8192 and columns <= 4096 else 2048
    start = first // tile
    mine = lambda at: pl.BlockSpec((rows, width), lambda j, b, at=at: (2 * at + (b[0] & 1), 0))
    span = lambda low, high: pl.BlockSpec((rows, tile), lambda j, b: (0, jnp.clip(start + j - low // tile, 0, (high - low) // tile - 1)))
    specs = [mine(at) for _ in range(2) for _, _, at in found]
    specs += [pl.BlockSpec((width, tile), lambda j, b: (0, start + j))] * 2
    adds = [a for a in adds if a[1] < first + columns and first < a[2]]
    whole = lambda low, high: low <= first and first + columns <= high
    return pl.pallas_call(
        functools.partial(_project, n=n, adds=tuple((i, low, high, whole(low, high)) for i, low, high, _ in adds),
                          outs=tuple((i, low, high, whole(low, high)) for i, low, high, _ in outs), start=start, tile=tile),
        grid_spec=pltpu.PrefetchScalarGridSpec(
            num_scalar_prefetch=1,
            grid=(columns // tile,),
            in_specs=specs + [span(low, high) for _, low, high, _ in adds],
            out_specs=[span(low, high) for _, low, high, _ in outs],
        ),
        out_shape=[jax.ShapeDtypeStruct((rows, high - low), kind) for _, low, high, kind in outs],
        compiler_params=pltpu.CompilerParams(dimension_semantics=("arbitrary",), vmem_limit_bytes=VMEM),
        cost_estimate=pl.CostEstimate(flops=4 * n * rows * width * columns, transcendentals=0,
                                      bytes_accessed=4 * width * columns + 4 * n * rows * (width + columns)),
        name="project",
    )(blocks, *[f[0] for f in found], *[f[1] for f in found], *weights, *[a[3] for a in adds])


def _sum(*refs, n):
    total = refs[0][...]
    for ref in refs[1:n]:
        total = total + ref[...].astype(jnp.float32)
    refs[-1][...] = total.astype(refs[-1].dtype)


def finish(terms, first, columns, before=None, tile=2048):
    rows, here = terms[0].shape
    start = first // tile
    given, specs, alias = list(terms), [pl.BlockSpec((rows, tile), lambda j: (0, j))] * len(terms), {}
    if before is not None:
        alias = {len(given): 0}
        given.append(before)
        specs.append(pl.BlockSpec(memory_space=pl.ANY))
    return pl.pallas_call(
        functools.partial(_sum, n=len(terms)),
        grid=(here // tile,),
        in_specs=specs,
        out_specs=pl.BlockSpec((rows, tile), lambda j: (0, start + j)),
        out_shape=jax.ShapeDtypeStruct((rows, columns), jnp.bfloat16),
        input_output_aliases=alias,
        compiler_params=pltpu.CompilerParams(dimension_semantics=("arbitrary",), vmem_limit_bytes=VMEM),
        cost_estimate=pl.CostEstimate(flops=rows * here * len(terms), transcendentals=0, bytes_accessed=12 * rows * here),
        name="finish",
    )(*given)


def solution(mesh):
    devices = mesh.shape["tp"]

    def hop(t, flip):
        pairs = [(i, i ^ flip) for i in range(devices)]
        return lax.ppermute(t, "tp", pairs)

    def step(x, gain, wq, wk, wv, wo):
        return body(x, gain, wq, wk, wv, wo)

    def body(x, gain, wq, wk, wv, wo):
        me = lax.axis_index("tp").astype(jnp.int32)
        rows, d = x.shape
        total = rows * devices
        third = d // 3
        half = rows // 2
        pair = [LINKS[l] | LINKS[l - 1] for l in range(3)]
        a = [normed(x[h * half : (h + 1) * half], gain) for h in range(2)]
        cos, sin = tables(total)
        tie = lax.optimization_barrier
        blocks = me ^ jnp.arange(devices, dtype=jnp.int32)

        near = [[hop(a[h], LINKS[l]) for l in range(3)] for h in range(2)]
        other = [hop(t, CORE) for t in a]

        def stage(found, before):
            places = tuple((flip, rows, row) for _, flip, row in found)
            return qkv_of([t for t, _, _ in found], places, blocks, wq, wk, wv, cos, sin, before)

        def own(ts, flips, row):
            return [(t, flip, row) for t, flip in zip(ts, flips)]

        def theirs(ts, flips, row):
            return [(hop(t, CORE), flip ^ CORE, row) for t, flip in zip(ts, flips)]

        def farthest(h):
            return [(hop(mid[h][(h + 2) % 3], LINKS[h]), FAR, h * half)]

        qkv = stage([(t, flip, h * half) for ts, flip in ((a, 0), (other, CORE)) for h, t in enumerate(ts)], None)
        near[0], qkv = tie((near[0], qkv))
        mid = [[hop(near[0][l - 1], LINKS[l]) for l in range(3)], None]
        late = theirs(near[0], LINKS, 0)
        qkv = stage(own(near[0], LINKS, 0), qkv)
        near[1], qkv = tie((near[1], qkv))
        mid[1] = [hop(near[1][l - 1], LINKS[l]) for l in range(3)]
        now, late = late + own(near[1], LINKS, half), theirs(near[1], LINKS, half)
        qkv = stage(now, qkv)
        mid[0], qkv, wo_in = tie((mid[0], qkv, wo))
        far = farthest(0)
        now, late = late + own(mid[0], pair, 0), theirs(mid[0], pair, 0)
        qkv = stage(now, qkv)
        mid[1], qkv = tie((mid[1], qkv))
        wo_other = hop(wo_in, CORE)
        far += farthest(1)
        now, late = late + own(mid[1], pair, half), theirs(mid[1], pair, half)
        qkv = stage(now, qkv)
        qkv = stage(late + far + [(hop(t, CORE), FAR ^ CORE, row) for t, _, row in far], qkv)

        weights = (wo, wo_other)

        def attended(flips):
            t = attention(qkv, flips, blocks, 2 * rows, 1024 if len(flips) == 1 else 512)
            other = hop(t, CORE)
            return {flip: (t, other, i) for i, flip in enumerate(flips)}

        seen = attended((FAR,))

        low, wide = jnp.bfloat16, jnp.float32
        thirds = [(l * third, (l + 1) * third) for l in range(3)]
        out = project([seen[FAR]], weights, blocks, [], [(0, *thirds[0], low)], 0, third)
        far_in = [hop(out[0], LINKS[0])]
        out = project([seen[FAR]], weights, blocks, [], [(0, *thirds[l], low) for l in (1, 2)], third, 2 * third)
        far_in += [hop(t, LINKS[l]) for l, t in zip((1, 2), out)]
        qkv, out = tie((qkv, out))
        seen |= attended(tuple(pair))
        mid_in, out = [], None
        for lo, hi in ((0, third), (third, d)):
            adds = [(l, (l + 1) % 3 * third, ((l + 1) % 3 + 1) * third, far_in[(l + 1) % 3]) for l in range(3)]
            out = project([seen[f] for f in pair], weights, blocks, adds, [(l, lo, hi, low) for l in range(3)], lo, hi - lo)
            mid_in.append([(lo, hi, hop(out[l], LINKS[l])) for l in range(3)])
        qkv, out = tie((qkv, out))
        seen |= attended((*LINKS, 0))
        rest, near_in = [], []
        for h, (lo, hi) in enumerate(thirds):
            adds = [(l, *mid_in[min(h, 1)][(l + 1) % 3]) for l in range(3)] + [(3, 0, d, x)]
            out = project([seen[f] for f in (*LINKS, 0)], weights, blocks, adds, [(l, lo, hi, low if l < 3 else wide) for l in range(4)], lo, hi - lo)
            near_in.append([hop(out[l], LINKS[l]) for l in range(3)])
            rest.append(out[3])
        y = None
        for h, (lo, _) in enumerate(thirds):
            y = finish([rest[h], *near_in[h]], lo, d, y)
        return y

    tokens, columns = P(("dp", "tp"), None), P(None, "tp")
    step = jax.shard_map(
        step,
        mesh=mesh,
        in_specs=(tokens, P(None), columns, columns, columns, P("tp", None)),
        out_specs=tokens,
        check_vma=False,
    )
    return step
```
